32 devices in a mesh: gx: 8 (over y, x, core), gy: 4 (over z).
Axes of the slice: x: 2, y: 2, z: 4, core: 2. Of those that a mesh axis runs over, the one named last changes fastest.
Arguments:
- point_feats: bfloat16 [262144, 128], P(('gx', 'gy')), may hold values from -6 to 6
- point_tile: int32 [262144, 1], P(('gx', 'gy')), may hold values from 0 to 31; in each aligned block of 8192 rows (0 to 8191, 8192 to 16383, ...) at most 320 rows name the same one
- point_cell: int32 [262144], P(('gx', 'gy')), may hold values from 0 to 4095
- point_count: int32 [32], P(('gx', 'gy')), may hold values from 6144 to 8192, as said below
- conv_weight: bfloat16 [3, 3, 128, 128], replicated, may hold values from -0.1875 to 0.1875
- conv_bias: float32 [128], replicated, may hold values from -3 to 3
Outputs:
- bev_map: bfloat16 [128, 1024, 128], P('gx', 'gy')
- conv_out: bfloat16 [128, 1024, 128], P('gx', 'gy')
The draws below stay inside these ranges and needn't reach their ends.
Inputs may be any that keep to these rules, and one draw needn't show every extreme that they name: `point_tile`: among the 8192 rows of one device no tile is named by more than 320 rows, a bound that some block reaches. `point_count`: only slots below a device's count are live; some device has all 8192 slots live.
All inputs are finite; a program needn't handle non-finite values.
Results may differ from the reference program's by a relative error of at most 0.0045.
Values may be sent and summed in bfloat16 or wider, within the bound.
A program may use at most 64 MiB of HBM per device.

```python
import math
import jax
import jax.numpy as jnp
import numpy as np
from jax import lax

C = 128
COLS_DEV = 256
ROWS_DEV = 16
P_DEV = 8192
CAP = 320
POINTS = 262144
MAP_ROWS = 128
MAP_COLS = 1024
N_GY = 4
DEVICES = 32


def draw_point_count(key, part):
    counts = jax.random.randint(key, (DEVICES,), 3 * P_DEV // 4, P_DEV + 1).astype(jnp.int32)
    fullest = jax.random.randint(jax.random.fold_in(key, 7), (), 0, DEVICES)
    return counts.at[fullest].set(P_DEV)


def with_ends(array, key, low, high):
    longest = array.shape.index(max(array.shape))
    spots = []
    for shift in (0, 1):
        where = [jax.random.randint(jax.random.fold_in(key, axis), (), 0, length) for axis, length in enumerate(array.shape)]
        where[longest] = (where[longest] + shift) % array.shape[longest]
        spots.append(tuple(where))
    return array.at[spots[0]].set(low).at[spots[1]].set(high)


def level_of(own_key, dims, cuts, low, largest):
    loudness, own = 1.0, jax.random.fold_in(own_key, 6)
    for dim, blocks in cuts:
        steps = jnp.exp(jax.random.uniform(jax.random.fold_in(own, dim), (blocks,), jnp.float32, low / len(cuts), largest / len(cuts)))
        loudness = loudness * jnp.repeat(steps, dims[dim] // blocks).reshape([-1 if axis == dim else 1 for axis in range(len(dims))])
    return loudness


def routed_block(own_key, own, number, rows, count, top, most, slope):
    sequence = jax.random.permutation(own_key, count)
    packed, usual = load_shares(count, rows * top, most, slope, True), load_shares(count, rows * top, most, slope, False)
    places = jnp.arange(count)

    def named(lengths, rotation):
        used = int((lengths > 0).sum())
        fixed = max(1, used // 4)
        passed = fixed + (places - fixed + rotation * (used - fixed)) % max(1, count - fixed)
        return jnp.zeros((count,), jnp.int32).at[sequence[jnp.where(places < fixed, places, passed)]].set(jnp.asarray(lengths, jnp.int32))

    lengths = jnp.where(number % 4 == 0, named(packed, number // 4), named(usual, number - number // 4 - 1))
    mixed = jax.random.permutation(jax.random.fold_in(own, 3), count)
    source_of, sink = mixed[0:count // 2 * 2:2], mixed[1:count // 2 * 2:2]
    margin = jnp.minimum(lengths[source_of] - 1, most - lengths[sink]) // 2
    margin = jnp.where((source_of == sequence[0]) | (sink == sequence[0]) | (lengths[sink] == 0), 0, jnp.maximum(margin, 0))
    passed = jax.random.randint(jax.random.fold_in(own, 4), (count // 2,), 0, 1 << 20) % (margin + 1)
    lengths = lengths.at[source_of].add(-passed).at[sink].add(passed)
    labels = jnp.searchsorted(jnp.cumsum(lengths), jnp.arange(rows * top), side="right").astype(jnp.int32)
    grid = labels.reshape(top, rows).T
    grid = grid[jax.random.permutation(jax.random.fold_in(own, 1), rows)]
    rotation = jax.random.randint(jax.random.fold_in(own, 2), (rows, 1), 0, top)
    return jnp.take_along_axis(grid, (jnp.arange(top)[None, :] + rotation) % top, axis=1)


def load_shares(number_of, total, bound, lean, full):
    loads = [(1 << 20) // math.isqrt(grade ** lean) + 1 for grade in range(1, number_of + 1)]
    largest = bound if full else min(bound, max(-(-total // number_of), total * loads[0] // sum(loads)))
    least = 1 if total - largest >= number_of - 1 else 0
    holding, spare = [largest] + [least] * (number_of - 1), total - largest - least * (number_of - 1)
    while spare > 0:
        candidates = [i for i in range(1, number_of) if holding[i] < largest] or [i for i in range(1, number_of) if holding[i] < bound]
        pool, left = sum([loads[i] for i in candidates]), spare
        for i in candidates:
            more = min(bound - holding[i], max(1, left * loads[i] // pool), spare)
            holding[i] = holding[i] + more
            spare = spare - more
    return np.array(holding)


def scatter_about(own_key, dims, deviation, reach, cuts=(), kind=jnp.bfloat16):
    drawn = jax.random.normal(own_key, dims, jnp.float32) * deviation
    if len(cuts) > 0:
        drawn = level_of(own_key, dims, cuts, -0.22, 0.18) * drawn
    return jnp.clip(drawn, min=-reach, max=reach).astype(kind)


def setup_inputs(seed: int = 0) -> dict:
    seeds = jax.random.split(jax.random.key(seed), 7)
    point_feats = scatter_about(seeds[0], (POINTS, C), 1.0, 6.0, ((0, 32),))
    point_tile_keys = jax.random.split(jax.random.fold_in(seeds[1], 1), POINTS // P_DEV)
    point_tile_turns = jax.random.permutation(jax.random.fold_in(seeds[1], 3), POINTS // P_DEV)
    point_tile = jax.vmap(lambda own, number: routed_block(jax.random.fold_in(seeds[1], 2), own, number, P_DEV, DEVICES, 1, CAP, 2))(point_tile_keys, point_tile_turns).reshape((POINTS, 1))
    point_cell = with_ends(jax.random.randint(seeds[2], (POINTS,), 0, ROWS_DEV * COLS_DEV), jax.random.fold_in(seeds[2], 1), 0, (ROWS_DEV * COLS_DEV) - 1).astype(jnp.int32)
    point_count = draw_point_count(jax.random.fold_in(seeds[6], 71), 0)
    conv_weight = scatter_about(seeds[4], (3, 3, C, C), (9 * C) ** -0.5, 0.1875)
    conv_bias = scatter_about(seeds[5], (C,), 0.5, 3.0, (), jnp.float32)
    return dict(point_feats=point_feats, point_tile=point_tile, point_cell=point_cell, point_count=point_count, conv_weight=conv_weight, conv_bias=conv_bias)


def reference(point_feats, point_tile, point_cell, point_count, conv_weight, conv_bias):
    tile = point_tile[:, 0]
    rows = (tile // N_GY) * ROWS_DEV + point_cell // COLS_DEV
    cols = (tile % N_GY) * COLS_DEV + point_cell % COLS_DEV
    cell = rows * MAP_COLS + cols
    slot = jnp.arange(POINTS, dtype=jnp.int32)
    block = slot // P_DEV
    live = (slot % P_DEV) < point_count[block]
    feats = jnp.where(live[:, None], point_feats.astype(jnp.float32), 0.0)
    sums = jax.ops.segment_sum(feats, cell, num_segments=MAP_ROWS * MAP_COLS)
    bev_map = sums.reshape(MAP_ROWS, MAP_COLS, C).astype(jnp.bfloat16)
    conv = lax.conv_general_dilated(bev_map.astype(jnp.float32)[None], conv_weight.astype(jnp.float32), (1, 1), "SAME", dimension_numbers=("NHWC", "HWIO", "NHWC"), precision=lax.Precision.HIGHEST)[0]
    conv_out = jax.nn.relu(conv + conv_bias).astype(jnp.bfloat16)
    return bev_map, conv_out
```

```python
import functools

import jax
import jax.numpy as jnp
from jax import lax
from jax.experimental import pallas as pl
from jax.experimental.pallas import tpu as pltpu
from jax.sharding import PartitionSpec as P

COLS_DEV = 256
ROWS_DEV = 16
CELLS = ROWS_DEV * COLS_DEV


def with_halo(cells, sides, width):
    for axis, dim in sides:
        count = lax.axis_size(axis)
        ends = count - 1
        head = lax.slice_in_dim(cells, 0, width, axis=dim)
        tail = lax.slice_in_dim(cells, cells.shape[dim] - width, cells.shape[dim], axis=dim)
        cells = jnp.concatenate(
            [
                lax.ppermute(tail, axis, [(i, (i + 1) % count) for i in range(ends)]),
                cells,
                lax.ppermute(head, axis, [((i + 1) % count, i) for i in range(ends)]),
            ],
            axis=dim,
        )
    return cells


def pack_kernel(stride, words, counts, feats, out, cells, fbuf, obuf):
    points = feats.shape[0]
    devices, capacity, _ = out.shape
    step = 512

    @pl.loop(0, points // step)
    def _(i):
        rows = pl.ds(pl.multiple_of(i * step, step), step)
        fbuf[rows, :] = feats[rows, :].astype(jnp.float32)

    @pl.loop(0, points // 16)
    def _(i):
        base = i * 16
        for j in range(16):
            word = words[base + j]
            pos = lax.shift_right_logical(word, 12)
            cells[pos] = word & (CELLS - 1)
            obuf[pl.ds(pos, 1), :] = fbuf[pl.ds(base + j, 1), :]

    @pl.loop(0, devices)
    def _(t):
        cells[t * stride + capacity] = counts[t]
        rows = pl.ds(pl.multiple_of(t * stride, stride), capacity)
        out[t] = obuf[rows, :].astype(jnp.bfloat16)


def pack(words, counts, feats, capacity, stride):
    devices = counts.shape[0]
    points, channels = feats.shape
    smem = pl.BlockSpec(memory_space=pltpu.SMEM)
    vmem = pl.BlockSpec(memory_space=pltpu.VMEM)
    return pl.pallas_call(
        functools.partial(pack_kernel, stride),
        out_shape=(
            jax.ShapeDtypeStruct((devices, capacity, channels), jnp.bfloat16),
            jax.ShapeDtypeStruct(((devices + 1) * stride,), jnp.int32),
        ),
        in_specs=[smem, smem, vmem],
        out_specs=(vmem, smem),
        scratch_shapes=[
            pltpu.VMEM((points, channels), jnp.float32),
            pltpu.VMEM((devices * stride + 8, channels), jnp.float32),
        ],
        compiler_params=pltpu.CompilerParams(vmem_limit_bytes=48 * 1024 * 1024),
        name="pack",
    )(words, counts, feats)


def scatter_kernel(feats, rows, cols, out, acc):
    step = pl.program_id(0)
    chunk = feats.shape[0]

    @pl.when(step == 0)
    def _():
        acc[...] = jnp.zeros_like(acc)

    ids = lax.broadcasted_iota(jnp.int32, (COLS_DEV, chunk), 0)
    onehot = jnp.where(ids == cols[0], 1.0, 0.0).astype(jnp.bfloat16)
    values = feats[...]
    row = rows[...]
    zero = jnp.zeros_like(values)
    for r in range(0, ROWS_DEV, 2):
        masked = jnp.concatenate(
            [jnp.where(row == jnp.bfloat16(r + k), values, zero) for k in range(2)], axis=1
        )
        part = jnp.dot(onehot, masked, preferred_element_type=jnp.float32)
        acc[:, r * 128 : (r + 2) * 128] += part

    @pl.when(step == pl.num_programs(0) - 1)
    def _():
        for r in range(ROWS_DEV):
            out[r] = acc[:, r * 128 : (r + 1) * 128].astype(jnp.bfloat16)


def scatter(feats, rows, cols, chunk):
    total, channels = feats.shape
    return pl.pallas_call(
        scatter_kernel,
        grid=(total // chunk,),
        out_shape=jax.ShapeDtypeStruct((ROWS_DEV, COLS_DEV, channels), jnp.bfloat16),
        in_specs=[
            pl.BlockSpec((chunk, channels), lambda i: (i, 0)),
            pl.BlockSpec((chunk, channels), lambda i: (i, 0)),
            pl.BlockSpec((1, 1, chunk), lambda i: (i, 0, 0)),
        ],
        out_specs=pl.BlockSpec((ROWS_DEV, COLS_DEV, channels), lambda i: (0, 0, 0)),
        scratch_shapes=[pltpu.VMEM((COLS_DEV, ROWS_DEV * channels), jnp.float32)],
        compiler_params=pltpu.CompilerParams(vmem_limit_bytes=48 * 1024 * 1024),
        name="scatter",
    )(feats, rows, cols.reshape(total // chunk, 1, chunk))


def places(target, live, devices):
    points = target.shape[0]
    blk = 256
    nblk = points // blk
    tile_ids = jnp.arange(devices, dtype=jnp.int32)
    hits = (tile_ids[:, None] == target[None, :]) & live[None, :]
    inner_idx = jnp.arange(blk, dtype=jnp.int32)
    upper = (inner_idx[:, None] <= inner_idx[None, :]).astype(jnp.bfloat16)
    blocks = hits.astype(jnp.bfloat16).reshape(devices, nblk, blk)
    inner = jnp.einsum("dbj,ji->dbi", blocks, upper, preferred_element_type=jnp.float32)
    totals = inner[:, :, -1]
    running = jnp.cumsum(totals, axis=1)
    ranks = inner + (running - totals)[:, :, None]
    place = jnp.sum(jnp.where(hits.reshape(devices, nblk, blk), ranks, 0.0), axis=0)
    return place.reshape(points).astype(jnp.int32) - 1, running[:, -1].astype(jnp.int32)


def shards(point_feats, point_tile, point_cell, point_count, conv_weight, conv_bias):
    size_gx = lax.axis_size("gx")
    size_gy = lax.axis_size("gy")
    devices = size_gx * size_gy
    points = point_feats.shape[0]
    channels = point_feats.shape[1]
    capacity = 5 * points // (4 * devices)
    stride = -(-(capacity + 1) // 128) * 128
    target = point_tile[:, 0]
    live = jnp.arange(points, dtype=jnp.int32) < point_count[0]
    place, counts = places(target, live, devices)
    position = jnp.where(live, target * stride + place, devices * stride)
    words = position * CELLS + point_cell
    send_feats, send_cells = pack(words, counts, point_feats, capacity, stride)
    got_cells = lax.all_to_all(
        send_cells[: devices * stride].reshape(devices, stride),
        ("gx", "gy"),
        split_axis=0,
        concat_axis=0,
        tiled=True,
    )
    got_feats = lax.all_to_all(
        send_feats, ("gx", "gy"), split_axis=0, concat_axis=0, tiled=True
    ).reshape(-1, channels)
    filled = jnp.arange(capacity, dtype=jnp.int32)[None, :] < got_cells[:, capacity : capacity + 1]
    cells = got_cells[:, :capacity]
    rows = jnp.where(filled, cells // COLS_DEV, -1).reshape(-1)
    cols = jnp.where(filled, cells % COLS_DEV, 0).reshape(-1)
    rows = jnp.broadcast_to(rows.astype(jnp.bfloat16)[:, None], got_feats.shape)
    bev_map = scatter(got_feats, rows, cols, devices * capacity // 8)
    padded = with_halo(bev_map, (("gx", 0), ("gy", 1)), 1)
    total = jnp.zeros((ROWS_DEV, COLS_DEV, channels), jnp.float32)
    for shift_row in range(3):
        for shift_col in range(3):
            window = padded[shift_row : shift_row + ROWS_DEV, shift_col : shift_col + COLS_DEV]
            total = total + jnp.einsum(
                "rcd,de->rce",
                window,
                conv_weight[shift_row, shift_col],
                preferred_element_type=jnp.float32,
            )
    conv_out = jax.nn.relu(total + conv_bias).astype(jnp.bfloat16)
    return (bev_map, conv_out)


def solution(mesh):
    in_specs = (
        P(("gx", "gy"), None),
        P(("gx", "gy"), None),
        P(("gx", "gy")),
        P(("gx", "gy")),
        P(),
        P(),
    )
    out_specs = (P("gx", "gy", None), P("gx", "gy", None))
    return jax.shard_map(shards, mesh=mesh, in_specs=in_specs, out_specs=out_specs, check_vma=False)
```

```python
import functools

import jax
import jax.numpy as jnp
from jax import lax
from jax.experimental import pallas as pl
from jax.experimental.pallas import tpu as pltpu
from jax.sharding import PartitionSpec as P

COLS_DEV = 256
ROWS_DEV = 16
CELLS = ROWS_DEV * COLS_DEV


def pack_kernel(stride, words, feats, out, cells, fbuf, obuf):
    points = feats.shape[0]
    devices, capacity, _ = out.shape
    step = 512

    @pl.loop(0, points // step)
    def _(i):
        rows = pl.ds(pl.multiple_of(i * step, step), step)
        fbuf[rows, :] = feats[rows, :].astype(jnp.float32)

    @pl.loop(0, points // 16)
    def _(i):
        base = i * 16
        for j in range(16):
            word = words[base + j]
            pos = lax.shift_right_logical(word, 12)
            cells[pos] = word & (CELLS - 1)
            obuf[pl.ds(pos, 1), :] = fbuf[pl.ds(base + j, 1), :]

    @pl.loop(0, devices)
    def _(t):
        rows = pl.ds(pl.multiple_of(t * stride, stride), capacity)
        out[t] = obuf[rows, :].astype(jnp.bfloat16)


def pack(words, feats, devices, capacity, stride):
    points, channels = feats.shape
    smem = pl.BlockSpec(memory_space=pltpu.SMEM)
    vmem = pl.BlockSpec(memory_space=pltpu.VMEM)
    return pl.pallas_call(
        functools.partial(pack_kernel, stride),
        out_shape=(
            jax.ShapeDtypeStruct((devices, capacity, channels), jnp.bfloat16),
            jax.ShapeDtypeStruct(((devices + 1) * stride,), jnp.int32),
        ),
        in_specs=[smem, vmem],
        out_specs=(vmem, smem),
        scratch_shapes=[
            pltpu.VMEM((points, channels), jnp.float32),
            pltpu.VMEM((devices * stride + 8, channels), jnp.float32),
        ],
        compiler_params=pltpu.CompilerParams(vmem_limit_bytes=48 * 1024 * 1024),
        name="pack",
    )(words, feats)


MESH = pl.DeviceIdType.MESH
GROUP = 4
NEIGHBOURS = [(dx, dy) for dx in (-1, 0, 1) for dy in (-1, 0, 1) if (dx, dy) != (0, 0)]


def map_kernel(
    size_gx,
    size_gy,
    send_feats,
    send_cells,
    weight,
    bias,
    bev,
    conv,
    got_feats,
    got_cells,
    acc,
    pad,
    edges,
    sides,
    flat,
    send_f,
    recv_f,
    send_c,
    recv_c,
    own,
    send_h,
    recv_h,
):
    devices = size_gx * size_gy
    capacity = send_feats.shape[1]
    gx, gy = lax.axis_index("gx"), lax.axis_index("gy")
    me = gx * size_gy + gy

    for r in (0, ROWS_DEV + 1):
        pad[r] = jnp.zeros_like(pad[r])
    sides[...] = jnp.zeros_like(sides)

    barrier = pltpu.get_barrier_semaphore()

    @pl.loop(1, devices)
    def _(k):
        other = lax.rem(me + k, devices)
        pl.semaphore_signal(
            barrier, inc=1, device_id=(other // size_gy, lax.rem(other, size_gy)), device_id_type=MESH
        )

    pl.semaphore_wait(barrier, devices - 1)

    def copies(source, owner, target):
        where = dict(
            device_id=(target // size_gy, lax.rem(target, size_gy)), device_id_type=MESH
        )
        return (
            pltpu.make_async_remote_copy(
                send_cells.at[source], got_cells.at[owner],
                send_c.at[source], recv_c.at[owner], **where,
            ),
            pltpu.make_async_remote_copy(
                send_feats.at[source], got_feats.at[owner, pl.ds(0, capacity)],
                send_f.at[source], recv_f.at[owner], **where,
            ),
        )

    @pl.loop(1, devices)
    def _(k):
        other = lax.rem(me + k, devices)
        for copy in copies(other, me, other):
            copy.start()

    mine = (
        pltpu.make_async_copy(send_cells.at[me], got_cells.at[me], own.at[0]),
        pltpu.make_async_copy(
            send_feats.at[me], got_feats.at[me, pl.ds(0, capacity)], own.at[1]
        ),
    )
    for copy in mine:
        copy.start()
    acc[...] = jnp.zeros_like(acc)
    for copy in mine:
        copy.wait()

    @pl.loop(0, devices // GROUP)
    def _(g):
        owners = [lax.rem(me + devices - (g * GROUP + j), devices) for j in range(GROUP)]
        for j, owner in enumerate(owners):

            @pl.when(g * GROUP + j > 0)
            def _():
                for copy in copies(owner, owner, owner):
                    copy.wait_recv()

        cells = jnp.concatenate([got_cells[owner] for owner in owners], axis=1)
        values = jnp.concatenate([got_feats[owner] for owner in owners], axis=0)
        length = cells.shape[1]
        row = jnp.right_shift(cells, 8).astype(jnp.float32)
        row = jnp.transpose(jnp.broadcast_to(row, (128, length))).astype(jnp.bfloat16)
        col = cells & (COLS_DEV - 1)
        ids = lax.broadcasted_iota(jnp.int32, (COLS_DEV, length), 0)
        onehot = jnp.where(ids == col, 1.0, 0.0).astype(jnp.bfloat16)
        zero = jnp.zeros_like(values)
        for r in range(0, ROWS_DEV, 2):
            masked = jnp.concatenate(
                [jnp.where(row == jnp.bfloat16(r + k), values, zero) for k in range(2)], axis=1
            )
            part = jnp.dot(onehot, masked, preferred_element_type=jnp.float32)
            acc[:, r * 128 : (r + 2) * 128] += part

    for r in range(ROWS_DEV):
        for side, c in ((0, 0), (1, COLS_DEV - 1)):
            edge = acc[c : c + 1, r * 128 : (r + 1) * 128]
            edges[side, r] = edge.astype(jnp.bfloat16).astype(jnp.float32)
    for r in range(ROWS_DEV):
        cells = acc[:, r * 128 : (r + 1) * 128].astype(jnp.bfloat16)
        pad[r + 1] = cells
        bev[r] = cells

    def inside(x, y):
        return (x >= 0) & (x < size_gx) & (y >= 0) & (y < size_gy)

    def halo(i):
        dx, dy = NEIGHBOURS[i]
        if dy == 0:
            src, dst = (pad.at[1], pad.at[ROWS_DEV + 1]) if dx < 0 else (pad.at[ROWS_DEV], pad.at[0])
        else:
            from_side, to_side = (0, 1) if dy < 0 else (1, 0)
            if dx == 0:
                src = edges.at[from_side]
                dst = sides.at[to_side, pl.ds(1, ROWS_DEV)]
            else:
                at = 0 if dx < 0 else ROWS_DEV - 1
                src = edges.at[from_side, pl.ds(at, 1)]
                dst = sides.at[to_side, pl.ds(ROWS_DEV + 1 if dx < 0 else 0, 1)]
        return pltpu.make_async_remote_copy(
            src, dst, send_h.at[i], recv_h.at[i], device_id=(gx + dx, gy + dy), device_id_type=MESH
        )

    for i, (dx, dy) in enumerate(NEIGHBOURS):

        @pl.when(inside(gx + dx, gy + dy))
        def _():
            halo(i).start()

    for i, (dx, dy) in enumerate(NEIGHBOURS):

        @pl.when(inside(gx - dx, gy - dy))
        def _():
            halo(i).wait_recv()

    side_sums = []
    for side in range(2):
        for r in range(ROWS_DEV + 2):
            flat[r : r + 1, :] = sides[side, r]
        near = jnp.concatenate([flat[a : a + ROWS_DEV, :] for a in range(3)], axis=1)
        taps = weight[:, :128] if side == 0 else weight[:, 256:]
        side_sums.append(
            jnp.dot(near.astype(jnp.bfloat16), taps, preferred_element_type=jnp.float32)
        )
    for side in range(2):
        flat[side * ROWS_DEV : (side + 1) * ROWS_DEV, :] = side_sums[side]
    place = lax.broadcasted_iota(jnp.int32, (COLS_DEV, 128), 0)

    @pl.loop(0, ROWS_DEV)
    def _(r):
        near = jnp.concatenate([pad[r + a] for a in range(3)], axis=1)
        sums = jnp.dot(near, weight[...], preferred_element_type=jnp.float32)
        left = jnp.where(place == 0, flat[pl.ds(r, 1), :], pltpu.roll(sums[:, :128], 1, 0))
        right = jnp.where(
            place == COLS_DEV - 1,
            flat[pl.ds(r + ROWS_DEV, 1), :],
            pltpu.roll(sums[:, 256:], COLS_DEV - 1, 0),
        )
        total = sums[:, 128:256] + left + right + bias[...]
        conv[r] = jnp.maximum(total, 0.0).astype(jnp.bfloat16)

    for i, (dx, dy) in enumerate(NEIGHBOURS):

        @pl.when(inside(gx + dx, gy + dy))
        def _():
            halo(i).wait_send()

    @pl.loop(1, devices)
    def _(k):
        other = lax.rem(me + k, devices)
        for copy in copies(other, me, other):
            copy.wait_send()


def make_map(feats, cells, weight, bias, size_gx, size_gy):
    devices, capacity, channels = feats.shape
    stride = cells.shape[-1]
    vmem = pl.BlockSpec(memory_space=pltpu.VMEM)
    shape = jax.ShapeDtypeStruct((ROWS_DEV, COLS_DEV, channels), jnp.bfloat16)
    dma = pltpu.SemaphoreType.DMA
    return pl.pallas_call(
        functools.partial(map_kernel, size_gx, size_gy),
        out_shape=(shape, shape),
        in_specs=[vmem] * 4,
        out_specs=(vmem, vmem),
        scratch_shapes=[
            pltpu.VMEM((devices, stride, channels), jnp.bfloat16),
            pltpu.VMEM((devices, 1, stride), jnp.int32),
            pltpu.VMEM((COLS_DEV, ROWS_DEV * channels), jnp.float32),
            pltpu.VMEM((ROWS_DEV + 2, COLS_DEV, channels), jnp.bfloat16),
            pltpu.VMEM((2, ROWS_DEV, 1, channels), jnp.float32),
            pltpu.VMEM((2, ROWS_DEV + 2, 1, channels), jnp.float32),
            pltpu.VMEM((2 * ROWS_DEV, channels), jnp.float32),
            dma((devices,)),
            dma((devices,)),
            dma((devices,)),
            dma((devices,)),
            dma((2,)),
            dma((len(NEIGHBOURS),)),
            dma((len(NEIGHBOURS),)),
        ],
        compiler_params=pltpu.CompilerParams(
            collective_id=0, has_side_effects=True, vmem_limit_bytes=56 * 1024 * 1024
        ),
        name="make_map",
    )(feats, cells, weight, bias)


def places(target, live, devices):
    points = target.shape[0]
    blk = 256
    nblk = points // blk
    tile_ids = jnp.arange(devices, dtype=jnp.int32)
    hits = (tile_ids[:, None] == target[None, :]) & live[None, :]
    inner_idx = jnp.arange(blk, dtype=jnp.int32)
    upper = (inner_idx[:, None] <= inner_idx[None, :]).astype(jnp.bfloat16)
    blocks = hits.astype(jnp.bfloat16).reshape(devices, nblk, blk)
    inner = jnp.einsum("dbj,ji->dbi", blocks, upper, preferred_element_type=jnp.float32)
    totals = inner[:, :, -1]
    running = jnp.cumsum(totals, axis=1)
    ranks = inner + (running - totals)[:, :, None]
    place = jnp.sum(jnp.where(hits.reshape(devices, nblk, blk), ranks, 0.0), axis=0)
    return place.reshape(points).astype(jnp.int32) - 1, running[:, -1].astype(jnp.int32)


def shards(point_feats, point_tile, point_cell, point_count, conv_weight, conv_bias):
    size_gx = lax.axis_size("gx")
    size_gy = lax.axis_size("gy")
    devices = size_gx * size_gy
    points = point_feats.shape[0]
    channels = point_feats.shape[1]
    capacity = 5 * points // (4 * devices)
    stride = -(-capacity // 128) * 128
    target = point_tile[:, 0]
    live = jnp.arange(points, dtype=jnp.int32) < point_count[0]
    place, counts = places(target, live, devices)
    position = jnp.where(live, target * stride + place, devices * stride)
    words = position * CELLS + point_cell
    send_feats, packed = pack(words, point_feats, devices, capacity, stride)
    filled = jnp.arange(stride, dtype=jnp.int32)[None, :] < counts[:, None]
    send_cells = jnp.where(filled, packed[: devices * stride].reshape(devices, stride), -1)
    taps = conv_weight.transpose(0, 2, 1, 3).reshape(3 * channels, 3 * channels)
    return make_map(
        send_feats,
        send_cells.reshape(devices, 1, stride),
        taps,
        conv_bias.reshape(1, channels),
        size_gx,
        size_gy,
    )


def solution(mesh):
    in_specs = (
        P(("gx", "gy"), None),
        P(("gx", "gy"), None),
        P(("gx", "gy")),
        P(("gx", "gy")),
        P(),
        P(),
    )
    out_specs = (P("gx", "gy", None), P("gx", "gy", None))
    return jax.shard_map(shards, mesh=mesh, in_specs=in_specs, out_specs=out_specs, check_vma=False)
```

```python
import functools

import jax
import jax.numpy as jnp
from jax import lax
from jax.experimental import pallas as pl
from jax.experimental.pallas import tpu as pltpu
from jax.sharding import PartitionSpec as P

COLS_DEV = 256
ROWS_DEV = 16
CELLS = ROWS_DEV * COLS_DEV


MESH = pl.DeviceIdType.MESH
GROUP = 4
CHUNK = 1024
NEIGHBOURS = [(dx, dy) for dx in (-1, 0, 1) for dy in (-1, 0, 1) if (dx, dy) != (0, 0)]


def map_kernel(
    size_gx,
    size_gy,
    feats,
    places,
    keys,
    weight,
    bias,
    bev,
    conv,
    slots,
    tiles,
    meta,
    send_feats,
    send_cells,
    got_feats,
    got_cells,
    acc,
    pad,
    edges,
    sides,
    flat,
    send_f,
    recv_f,
    send_c,
    recv_c,
    own,
    send_h,
    recv_h,
):
    devices = size_gx * size_gy
    capacity = send_feats.shape[1]
    gx, gy = lax.axis_index("gx"), lax.axis_index("gy")
    me = gx * size_gy + gy

    for r in (0, ROWS_DEV + 1):
        pad[r] = jnp.zeros_like(pad[r])
    sides[...] = jnp.zeros_like(sides)

    barrier = pltpu.get_barrier_semaphore()

    @pl.loop(1, devices)
    def _(k):
        other = lax.rem(me + k, devices)
        pl.semaphore_signal(
            barrier, inc=1, device_id=(other // size_gy, lax.rem(other, size_gy)), device_id_type=MESH
        )

    chunks = places.shape[0]
    stride = got_feats.shape[1]

    @pl.loop(0, chunks)
    def _(c):
        rows = pl.ds(pl.multiple_of(c * CHUNK, CHUNK), CHUNK)
        ids = lax.broadcasted_iota(jnp.int32, (capacity, CHUNK), 0)
        slots[c] = jnp.where(ids == places[c], 1.0, 0.0).astype(jnp.bfloat16)
        key = jnp.transpose(jnp.broadcast_to(keys[c], (128, CHUNK))).astype(jnp.int32)
        tile = jnp.right_shift(key, 12)
        tiles[rows, :] = tile.astype(jnp.float32).astype(jnp.bfloat16)
        hit = tile == lax.broadcasted_iota(jnp.int32, (CHUNK, 128), 1)
        row = (jnp.right_shift(key, 8) & (ROWS_DEV - 1)) + 1
        col = key & (COLS_DEV - 1)
        for at, part in ((0, row), (128, col)):
            part = jnp.where(hit, part, 0).astype(jnp.float32)
            meta[rows, at : at + 128] = part.astype(jnp.bfloat16)

    def packed(operand):
        total = None
        for c in range(chunks):
            part = jnp.dot(slots[c], operand(c), preferred_element_type=jnp.float32)
            total = part if total is None else total + part
        return total

    found = packed(lambda c: meta[c * CHUNK : (c + 1) * CHUNK, :])
    found = found[:, :128] * 256.0 + found[:, 128:]
    if stride > capacity:
        found = jnp.concatenate([found, jnp.zeros((stride - capacity, 128), jnp.float32)], axis=0)
    found = jnp.transpose(found)
    for t in range(devices):
        send_cells[t] = found[t : t + 1, :]

    pl.semaphore_wait(barrier, devices - 1)

    def copies(source, owner, target):
        where = dict(
            device_id=(target // size_gy, lax.rem(target, size_gy)), device_id_type=MESH
        )
        return (
            pltpu.make_async_remote_copy(
                send_cells.at[source], got_cells.at[owner],
                send_c.at[source], recv_c.at[owner], **where,
            ),
            pltpu.make_async_remote_copy(
                send_feats.at[source], got_feats.at[owner, pl.ds(0, capacity)],
                send_f.at[source], recv_f.at[owner], **where,
            ),
        )

    mine = (
        pltpu.make_async_copy(send_cells.at[me], got_cells.at[me], own.at[0]),
        pltpu.make_async_copy(
            send_feats.at[me], got_feats.at[me, pl.ds(0, capacity)], own.at[1]
        ),
    )
    pairs = devices // 2
    half = me // 2

    def send(q):
        pair = lax.rem(half + q, pairs)
        for k in range(2):
            target = pair * 2 + k

            @pl.when(target != me)
            def _():
                for copy in copies(target, me, target):
                    copy.start()

            @pl.when(target == me)
            def _():
                for copy in mine:
                    copy.start()

    @pl.loop(0, pairs)
    def _(q):
        pair = lax.rem(half + q, pairs)
        names = [(pair * 2 + k).astype(jnp.float32).astype(jnp.bfloat16) for k in range(2)]

        def masked(c):
            rows = slice(c * CHUNK, (c + 1) * CHUNK)
            values, tile = feats[rows, :], tiles[rows, :]
            zero = jnp.zeros_like(values)
            return jnp.concatenate([jnp.where(tile == n, values, zero) for n in names], axis=1)

        block = packed(masked).astype(jnp.bfloat16)
        for k in range(2):
            send_feats[pair * 2 + k] = block[:, k * 128 : (k + 1) * 128]

        @pl.when(q > 0)
        def _():
            send(q - 1)

    send(pairs - 1)
    acc[...] = jnp.zeros_like(acc)

    @pl.loop(0, devices // GROUP)
    def _(g):
        owners = []
        for j in range(GROUP // 2):
            pair = lax.rem(half + pairs - (g * (GROUP // 2) + j), pairs)
            owners += [pair * 2, pair * 2 + 1]
        for owner in owners:

            @pl.when(owner != me)
            def _():
                for copy in copies(owner, owner, owner):
                    copy.wait_recv()

            @pl.when(owner == me)
            def _():
                for copy in mine:
                    copy.wait()

        cells = jnp.concatenate([got_cells[owner] for owner in owners], axis=1).astype(jnp.int32)
        values = jnp.concatenate([got_feats[owner] for owner in owners], axis=0)
        length = cells.shape[1]
        row = (jnp.right_shift(cells, 8) - 1).astype(jnp.float32)
        row = jnp.transpose(jnp.broadcast_to(row, (128, length))).astype(jnp.bfloat16)
        col = cells & (COLS_DEV - 1)
        ids = lax.broadcasted_iota(jnp.int32, (COLS_DEV, length), 0)
        onehot = jnp.where(ids == col, 1.0, 0.0).astype(jnp.bfloat16)
        zero = jnp.zeros_like(values)
        for r in range(0, ROWS_DEV, 2):
            masked = jnp.concatenate(
                [jnp.where(row == jnp.bfloat16(r + k), values, zero) for k in range(2)], axis=1
            )
            part = jnp.dot(onehot, masked, preferred_element_type=jnp.float32)
            acc[:, r * 128 : (r + 2) * 128] += part

    for r in range(ROWS_DEV):
        for side, c in ((0, 0), (1, COLS_DEV - 1)):
            edge = acc[c : c + 1, r * 128 : (r + 1) * 128]
            edges[side, r] = edge.astype(jnp.bfloat16).astype(jnp.float32)
    for r in range(ROWS_DEV):
        cells = acc[:, r * 128 : (r + 1) * 128].astype(jnp.bfloat16)
        pad[r + 1] = cells
        bev[r] = cells

    def inside(x, y):
        return (x >= 0) & (x < size_gx) & (y >= 0) & (y < size_gy)

    def halo(i):
        dx, dy = NEIGHBOURS[i]
        if dy == 0:
            src, dst = (pad.at[1], pad.at[ROWS_DEV + 1]) if dx < 0 else (pad.at[ROWS_DEV], pad.at[0])
        else:
            from_side, to_side = (0, 1) if dy < 0 else (1, 0)
            if dx == 0:
                src = edges.at[from_side]
                dst = sides.at[to_side, pl.ds(1, ROWS_DEV)]
            else:
                at = 0 if dx < 0 else ROWS_DEV - 1
                src = edges.at[from_side, pl.ds(at, 1)]
                dst = sides.at[to_side, pl.ds(ROWS_DEV + 1 if dx < 0 else 0, 1)]
        return pltpu.make_async_remote_copy(
            src, dst, send_h.at[i], recv_h.at[i], device_id=(gx + dx, gy + dy), device_id_type=MESH
        )

    for i, (dx, dy) in enumerate(NEIGHBOURS):

        @pl.when(inside(gx + dx, gy + dy))
        def _():
            halo(i).start()

    for i, (dx, dy) in enumerate(NEIGHBOURS):

        @pl.when(inside(gx - dx, gy - dy))
        def _():
            halo(i).wait_recv()

    side_sums = []
    for side in range(2):
        for r in range(ROWS_DEV + 2):
            flat[r : r + 1, :] = sides[side, r]
        near = jnp.concatenate([flat[a : a + ROWS_DEV, :] for a in range(3)], axis=1)
        taps = weight[:, :128] if side == 0 else weight[:, 256:]
        side_sums.append(
            jnp.dot(near.astype(jnp.bfloat16), taps, preferred_element_type=jnp.float32)
        )
    for side in range(2):
        flat[side * ROWS_DEV : (side + 1) * ROWS_DEV, :] = side_sums[side]
    place = lax.broadcasted_iota(jnp.int32, (COLS_DEV, 128), 0)

    @pl.loop(0, ROWS_DEV)
    def _(r):
        near = jnp.concatenate([pad[r + a] for a in range(3)], axis=1)
        sums = jnp.dot(near, weight[...], preferred_element_type=jnp.float32)
        left = jnp.where(place == 0, flat[pl.ds(r, 1), :], pltpu.roll(sums[:, :128], 1, 0))
        right = jnp.where(
            place == COLS_DEV - 1,
            flat[pl.ds(r + ROWS_DEV, 1), :],
            pltpu.roll(sums[:, 256:], COLS_DEV - 1, 0),
        )
        total = sums[:, 128:256] + left + right + bias[...]
        conv[r] = jnp.maximum(total, 0.0).astype(jnp.bfloat16)

    for i, (dx, dy) in enumerate(NEIGHBOURS):

        @pl.when(inside(gx + dx, gy + dy))
        def _():
            halo(i).wait_send()

    @pl.loop(1, devices)
    def _(k):
        other = lax.rem(me + k, devices)
        for copy in copies(other, me, other):
            copy.wait_send()


def make_map(feats, places, keys, weight, bias, size_gx, size_gy, capacity):
    devices = size_gx * size_gy
    points, channels = feats.shape
    stride = -(-capacity // 128) * 128
    vmem = pl.BlockSpec(memory_space=pltpu.VMEM)
    shape = jax.ShapeDtypeStruct((ROWS_DEV, COLS_DEV, channels), jnp.bfloat16)
    dma = pltpu.SemaphoreType.DMA
    return pl.pallas_call(
        functools.partial(map_kernel, size_gx, size_gy),
        out_shape=(shape, shape),
        in_specs=[vmem] * 5,
        out_specs=(vmem, vmem),
        scratch_shapes=[
            pltpu.VMEM((points // CHUNK, capacity, CHUNK), jnp.bfloat16),
            pltpu.VMEM((points, 128), jnp.bfloat16),
            pltpu.VMEM((points, 256), jnp.bfloat16),
            pltpu.VMEM((devices, capacity, channels), jnp.bfloat16),
            pltpu.VMEM((devices, 1, stride), jnp.float32),
            pltpu.VMEM((devices, stride, channels), jnp.bfloat16),
            pltpu.VMEM((devices, 1, stride), jnp.float32),
            pltpu.VMEM((COLS_DEV, ROWS_DEV * channels), jnp.float32),
            pltpu.VMEM((ROWS_DEV + 2, COLS_DEV, channels), jnp.bfloat16),
            pltpu.VMEM((2, ROWS_DEV, 1, channels), jnp.float32),
            pltpu.VMEM((2, ROWS_DEV + 2, 1, channels), jnp.float32),
            pltpu.VMEM((2 * ROWS_DEV, channels), jnp.float32),
            dma((devices,)),
            dma((devices,)),
            dma((devices,)),
            dma((devices,)),
            dma((2,)),
            dma((len(NEIGHBOURS),)),
            dma((len(NEIGHBOURS),)),
        ],
        compiler_params=pltpu.CompilerParams(
            collective_id=0, has_side_effects=True, vmem_limit_bytes=56 * 1024 * 1024
        ),
        name="make_map",
    )(feats, places, keys, weight, bias)


def places(target, live, devices):
    points = target.shape[0]
    blk = 256
    nblk = points // blk
    tile_ids = jnp.arange(devices, dtype=jnp.int32)
    hits = (tile_ids[:, None] == target[None, :]) & live[None, :]
    inner_idx = jnp.arange(blk, dtype=jnp.int32)
    upper = (inner_idx[:, None] <= inner_idx[None, :]).astype(jnp.bfloat16)
    blocks = hits.astype(jnp.bfloat16).reshape(devices, nblk, blk)
    inner = jnp.einsum("dbj,ji->dbi", blocks, upper, preferred_element_type=jnp.float32)
    totals = inner[:, :, -1]
    running = jnp.cumsum(totals, axis=1)
    ranks = inner + (running - totals)[:, :, None]
    place = jnp.sum(jnp.where(hits.reshape(devices, nblk, blk), ranks, 0.0), axis=0)
    return place.reshape(points).astype(jnp.int32) - 1


def shards(point_feats, point_tile, point_cell, point_count, conv_weight, conv_bias):
    size_gx = lax.axis_size("gx")
    size_gy = lax.axis_size("gy")
    devices = size_gx * size_gy
    points = point_feats.shape[0]
    channels = point_feats.shape[1]
    capacity = 5 * points // (4 * devices)
    target = point_tile[:, 0]
    live = jnp.arange(points, dtype=jnp.int32) < point_count[0]
    place = places(target, live, devices)
    keys = jnp.where(live, target, devices) * CELLS + point_cell
    taps = conv_weight.transpose(0, 2, 1, 3).reshape(3 * channels, 3 * channels)
    return make_map(
        point_feats,
        place.reshape(-1, 1, CHUNK),
        keys.astype(jnp.float32).reshape(-1, 1, CHUNK),
        taps,
        conv_bias.reshape(1, channels),
        size_gx,
        size_gy,
        capacity,
    )


def solution(mesh):
    in_specs = (
        P(("gx", "gy"), None),
        P(("gx", "gy"), None),
        P(("gx", "gy")),
        P(("gx", "gy")),
        P(),
        P(),
    )
    out_specs = (P("gx", "gy", None), P("gx", "gy", None))
    return jax.shard_map(shards, mesh=mesh, in_specs=in_specs, out_specs=out_specs, check_vma=False)
```

```python
import functools

import jax
import jax.numpy as jnp
from jax import lax
from jax.experimental import pallas as pl
from jax.experimental.pallas import tpu as pltpu
from jax.sharding import PartitionSpec as P

COLS_DEV = 256
ROWS_DEV = 16
CELLS = ROWS_DEV * COLS_DEV


MESH = pl.DeviceIdType.MESH
GROUP = 4
CHUNK = 1024
NEIGHBOURS = [(dx, dy) for dx in (-1, 0, 1) for dy in (-1, 0, 1) if (dx, dy) != (0, 0)]


def map_kernel(
    size_gx,
    size_gy,
    feats,
    keys,
    taps,
    bias,
    bev,
    conv,
    weight,
    slots,
    tiles,
    meta,
    send_feats,
    send_cells,
    got_feats,
    got_cells,
    acc,
    pad,
    edges,
    sides,
    flat,
    send_f,
    recv_f,
    send_c,
    recv_c,
    own,
    send_h,
    recv_h,
):
    devices = size_gx * size_gy
    capacity = send_feats.shape[1]
    gx, gy = lax.axis_index("gx"), lax.axis_index("gy")
    me = gx * size_gy + gy

    for r in (0, ROWS_DEV + 1):
        pad[r] = jnp.zeros_like(pad[r])
    sides[...] = jnp.zeros_like(sides)

    barrier = pltpu.get_barrier_semaphore()

    @pl.loop(1, devices)
    def _(k):
        other = lax.rem(me + k, devices)
        pl.semaphore_signal(
            barrier, inc=1, device_id=(other // size_gy, lax.rem(other, size_gy)), device_id_type=MESH
        )

    chunks = keys.shape[0]
    stride = got_feats.shape[1]

    for a in range(3):
        for b in range(3):
            weight[a * 128 : (a + 1) * 128, b * 128 : (b + 1) * 128] = taps[a, b]
    inner = 256
    upper = lax.broadcasted_iota(jnp.int32, (inner, inner), 0) <= lax.broadcasted_iota(
        jnp.int32, (inner, inner), 1
    )
    upper = jnp.where(upper, 1.0, 0.0).astype(jnp.bfloat16)
    names = lax.broadcasted_iota(jnp.int32, (devices, inner), 0)

    def prepare(c, before):
        target = jnp.right_shift(keys[c].astype(jnp.int32), 12)
        found = []
        for at in range(0, CHUNK, inner):
            hits = jnp.where(names == target[:, at : at + inner], 1.0, 0.0)
            ranks = jnp.dot(hits.astype(jnp.bfloat16), upper, preferred_element_type=jnp.float32)
            found.append(jnp.sum(hits * (ranks + before), axis=0, keepdims=True) - 1.0)
            before = before + jnp.sum(hits, axis=1, keepdims=True)
        place = jnp.concatenate(found, axis=1).astype(jnp.int32)
        rows = pl.ds(pl.multiple_of(c * CHUNK, CHUNK), CHUNK)
        ids = lax.broadcasted_iota(jnp.int32, (capacity, CHUNK), 0)
        slots[c] = jnp.where(ids == place, 1.0, 0.0).astype(jnp.bfloat16)
        key = jnp.transpose(jnp.broadcast_to(keys[c], (128, CHUNK))).astype(jnp.int32)
        tile = jnp.right_shift(key, 12)
        tiles[rows, :] = tile.astype(jnp.float32).astype(jnp.bfloat16)
        hit = tile == lax.broadcasted_iota(jnp.int32, (CHUNK, 128), 1)
        row = (jnp.right_shift(key, 8) & (ROWS_DEV - 1)) + 1
        col = key & (COLS_DEV - 1)
        for at, part in ((0, row), (128, col)):
            part = jnp.where(hit, part, 0).astype(jnp.float32)
            meta[rows, at : at + 128] = part.astype(jnp.bfloat16)
        return before

    lax.fori_loop(0, chunks, prepare, jnp.zeros((devices, inner), jnp.float32))

    def packed(operand):
        total = None
        for c in range(chunks):
            part = jnp.dot(slots[c], operand(c), preferred_element_type=jnp.float32)
            total = part if total is None else total + part
        return total

    found = packed(lambda c: meta[c * CHUNK : (c + 1) * CHUNK, :])
    found = found[:, :128] * 256.0 + found[:, 128:]
    if stride > capacity:
        found = jnp.concatenate([found, jnp.zeros((stride - capacity, 128), jnp.float32)], axis=0)
    found = jnp.transpose(found)
    for t in range(devices):
        send_cells[t] = found[t : t + 1, :]

    pl.semaphore_wait(barrier, devices - 1)

    def copies(source, owner, target):
        where = dict(
            device_id=(target // size_gy, lax.rem(target, size_gy)), device_id_type=MESH
        )
        return (
            pltpu.make_async_remote_copy(
                send_cells.at[source], got_cells.at[owner],
                send_c.at[source], recv_c.at[owner], **where,
            ),
            pltpu.make_async_remote_copy(
                send_feats.at[source], got_feats.at[owner, pl.ds(0, capacity)],
                send_f.at[source], recv_f.at[owner], **where,
            ),
        )

    mine = (
        pltpu.make_async_copy(send_cells.at[me], got_cells.at[me], own.at[0]),
        pltpu.make_async_copy(
            send_feats.at[me], got_feats.at[me, pl.ds(0, capacity)], own.at[1]
        ),
    )
    pairs = devices // 2
    half = me // 2

    def offset(q):
        return lax.rem(2 * q + 1, pairs) - q // (pairs // 2)

    def send(q):
        pair = lax.rem(half + offset(q), pairs)
        for k in range(2):
            target = pair * 2 + k

            @pl.when(target != me)
            def _():
                for copy in copies(target, me, target):
                    copy.start()

            @pl.when(target == me)
            def _():
                for copy in mine:
                    copy.start()

    @pl.loop(0, pairs)
    def _(q):
        pair = lax.rem(half + offset(q), pairs)
        names = [(pair * 2 + k).astype(jnp.float32).astype(jnp.bfloat16) for k in range(2)]

        def masked(c):
            rows = slice(c * CHUNK, (c + 1) * CHUNK)
            values, tile = feats[rows, :], tiles[rows, :]
            zero = jnp.zeros_like(values)
            return jnp.concatenate([jnp.where(tile == n, values, zero) for n in names], axis=1)

        block = packed(masked).astype(jnp.bfloat16)
        for k in range(2):
            send_feats[pair * 2 + k] = block[:, k * 128 : (k + 1) * 128]

        @pl.when(q > 0)
        def _():
            send(q - 1)

    send(pairs - 1)
    acc[...] = jnp.zeros_like(acc)

    @pl.loop(0, devices // GROUP)
    def _(g):
        owners = []
        for j in range(GROUP // 2):
            q = lax.rem(g * (GROUP // 2) + j + pairs // 2, pairs)
            pair = lax.rem(half + pairs - offset(q), pairs)
            owners += [pair * 2, pair * 2 + 1]
        for owner in owners:

            @pl.when(owner != me)
            def _():
                for copy in copies(owner, owner, owner):
                    copy.wait_recv()

            @pl.when(owner == me)
            def _():
                for copy in mine:
                    copy.wait()

        cells = jnp.concatenate([got_cells[owner] for owner in owners], axis=1).astype(jnp.int32)
        values = jnp.concatenate([got_feats[owner] for owner in owners], axis=0)
        length = cells.shape[1]
        row = (jnp.right_shift(cells, 8) - 1).astype(jnp.float32)
        row = jnp.transpose(jnp.broadcast_to(row, (128, length))).astype(jnp.bfloat16)
        col = cells & (COLS_DEV - 1)
        ids = lax.broadcasted_iota(jnp.int32, (COLS_DEV, length), 0)
        onehot = jnp.where(ids == col, 1.0, 0.0).astype(jnp.bfloat16)
        zero = jnp.zeros_like(values)
        for r in range(0, ROWS_DEV, 2):
            masked = jnp.concatenate(
                [jnp.where(row == jnp.bfloat16(r + k), values, zero) for k in range(2)], axis=1
            )
            part = jnp.dot(onehot, masked, preferred_element_type=jnp.float32)
            acc[:, r * 128 : (r + 2) * 128] += part

    for r in range(ROWS_DEV):
        for side, c in ((0, 0), (1, COLS_DEV - 1)):
            edge = acc[c : c + 1, r * 128 : (r + 1) * 128]
            edges[side, r] = edge.astype(jnp.bfloat16).astype(jnp.float32)
    for r in range(ROWS_DEV):
        cells = acc[:, r * 128 : (r + 1) * 128].astype(jnp.bfloat16)
        pad[r + 1] = cells
        bev[r] = cells

    def inside(x, y):
        return (x >= 0) & (x < size_gx) & (y >= 0) & (y < size_gy)

    def halo(i):
        dx, dy = NEIGHBOURS[i]
        if dy == 0:
            src, dst = (pad.at[1], pad.at[ROWS_DEV + 1]) if dx < 0 else (pad.at[ROWS_DEV], pad.at[0])
        else:
            from_side, to_side = (0, 1) if dy < 0 else (1, 0)
            if dx == 0:
                src = edges.at[from_side]
                dst = sides.at[to_side, pl.ds(1, ROWS_DEV)]
            else:
                at = 0 if dx < 0 else ROWS_DEV - 1
                src = edges.at[from_side, pl.ds(at, 1)]
                dst = sides.at[to_side, pl.ds(ROWS_DEV + 1 if dx < 0 else 0, 1)]
        return pltpu.make_async_remote_copy(
            src, dst, send_h.at[i], recv_h.at[i], device_id=(gx + dx, gy + dy), device_id_type=MESH
        )

    for i, (dx, dy) in enumerate(NEIGHBOURS):

        @pl.when(inside(gx + dx, gy + dy))
        def _():
            halo(i).start()

    for i, (dx, dy) in enumerate(NEIGHBOURS):

        @pl.when(inside(gx - dx, gy - dy))
        def _():
            halo(i).wait_recv()

    side_sums = []
    for side in range(2):
        for r in range(ROWS_DEV + 2):
            flat[r : r + 1, :] = sides[side, r]
        near = jnp.concatenate([flat[a : a + ROWS_DEV, :] for a in range(3)], axis=1)
        taps = weight[:, :128] if side == 0 else weight[:, 256:]
        side_sums.append(
            jnp.dot(near.astype(jnp.bfloat16), taps, preferred_element_type=jnp.float32)
        )
    for side in range(2):
        flat[side * ROWS_DEV : (side + 1) * ROWS_DEV, :] = side_sums[side]
    place = lax.broadcasted_iota(jnp.int32, (COLS_DEV, 128), 0)

    @pl.loop(0, ROWS_DEV)
    def _(r):
        near = jnp.concatenate([pad[r + a] for a in range(3)], axis=1)
        sums = jnp.dot(near, weight[...], preferred_element_type=jnp.float32)
        left = jnp.where(place == 0, flat[pl.ds(r, 1), :], pltpu.roll(sums[:, :128], 1, 0))
        right = jnp.where(
            place == COLS_DEV - 1,
            flat[pl.ds(r + ROWS_DEV, 1), :],
            pltpu.roll(sums[:, 256:], COLS_DEV - 1, 0),
        )
        total = sums[:, 128:256] + left + right + bias[...]
        conv[r] = jnp.maximum(total, 0.0).astype(jnp.bfloat16)

    for i, (dx, dy) in enumerate(NEIGHBOURS):

        @pl.when(inside(gx + dx, gy + dy))
        def _():
            halo(i).wait_send()

    @pl.loop(1, devices)
    def _(k):
        other = lax.rem(me + k, devices)
        for copy in copies(other, me, other):
            copy.wait_send()


def make_map(feats, keys, weight, bias, size_gx, size_gy, capacity):
    devices = size_gx * size_gy
    points, channels = feats.shape
    stride = -(-capacity // 128) * 128
    vmem = pl.BlockSpec(memory_space=pltpu.VMEM)
    shape = jax.ShapeDtypeStruct((ROWS_DEV, COLS_DEV, channels), jnp.bfloat16)
    dma = pltpu.SemaphoreType.DMA
    return pl.pallas_call(
        functools.partial(map_kernel, size_gx, size_gy),
        out_shape=(shape, shape),
        in_specs=[vmem] * 4,
        out_specs=(vmem, vmem),
        scratch_shapes=[
            pltpu.VMEM((3 * channels, 3 * channels), jnp.bfloat16),
            pltpu.VMEM((points // CHUNK, capacity, CHUNK), jnp.bfloat16),
            pltpu.VMEM((points, 128), jnp.bfloat16),
            pltpu.VMEM((points, 256), jnp.bfloat16),
            pltpu.VMEM((devices, capacity, channels), jnp.bfloat16),
            pltpu.VMEM((devices, 1, stride), jnp.float32),
            pltpu.VMEM((devices, stride, channels), jnp.bfloat16),
            pltpu.VMEM((devices, 1, stride), jnp.float32),
            pltpu.VMEM((COLS_DEV, ROWS_DEV * channels), jnp.float32),
            pltpu.VMEM((ROWS_DEV + 2, COLS_DEV, channels), jnp.bfloat16),
            pltpu.VMEM((2, ROWS_DEV, 1, channels), jnp.float32),
            pltpu.VMEM((2, ROWS_DEV + 2, 1, channels), jnp.float32),
            pltpu.VMEM((2 * ROWS_DEV, channels), jnp.float32),
            dma((devices,)),
            dma((devices,)),
            dma((devices,)),
            dma((devices,)),
            dma((2,)),
            dma((len(NEIGHBOURS),)),
            dma((len(NEIGHBOURS),)),
        ],
        compiler_params=pltpu.CompilerParams(
            collective_id=0, has_side_effects=True, vmem_limit_bytes=56 * 1024 * 1024
        ),
        name="make_map",
    )(feats, keys, weight, bias)


def shards(point_feats, point_tile, point_cell, point_count, conv_weight, conv_bias):
    size_gx = lax.axis_size("gx")
    size_gy = lax.axis_size("gy")
    devices = size_gx * size_gy
    points = point_feats.shape[0]
    channels = point_feats.shape[1]
    capacity = 5 * points // (4 * devices)
    target = point_tile[:, 0]
    live = jnp.arange(points, dtype=jnp.int32) < point_count[0]
    keys = jnp.where(live, target, devices) * CELLS + point_cell
    return make_map(
        point_feats,
        keys.astype(jnp.float32).reshape(-1, 1, CHUNK),
        conv_weight,
        conv_bias.reshape(1, channels),
        size_gx,
        size_gy,
        capacity,
    )


def solution(mesh):
    in_specs = (
        P(("gx", "gy"), None),
        P(("gx", "gy"), None),
        P(("gx", "gy")),
        P(("gx", "gy")),
        P(),
        P(),
    )
    out_specs = (P("gx", "gy", None), P("gx", "gy", None))
    return jax.shard_map(shards, mesh=mesh, in_specs=in_specs, out_specs=out_specs, check_vma=False)
```
